32 devices in a mesh: row: 8 (over y, x, core), col: 4 (over z).
Axes of the slice: x: 2, y: 2, z: 4, core: 2. Of those that a mesh axis runs over, the one named last changes fastest.
Arguments:
- pair_factors: float32 [12288, 1024], P(('row', 'col')), may hold values from -0.09375 to 0.09375
- k_prev: float32 [12288, 12288], P('row', 'col'), as said below
- energies: float32 [12288], P('row'), may hold values from 0.3 to 2
Outputs:
- casida: float32 [12288, 12288], P('row', 'col')
- vectors: float32 [12288, 8], P('row')
- images: float32 [12288, 8], P('row')
- tridiagonal: float32 [2, 8], replicated
The draws below stay inside these ranges and needn't reach their ends.
Inputs may be any that keep to these rules, and one draw needn't show every extreme that they name: k_prev is exactly symmetric.
All inputs are finite; a program needn't handle non-finite values.
Results may differ from the reference program's by a relative error of at most 0.0003.
Values sent between devices are 32-bit elements; how exact they have to be, the bound alone decides.
No kernel may reach another device: no remote copies, remote signals or barrier semaphores. Data moves between devices by JAX's collectives and lax.ppermute only.
A program may use at most 128 MiB of HBM per device.

```python
import math
import jax
import jax.numpy as jnp
from jax import lax

N = 12288
PC = 8
AUXW = 1024


def draw_k_prev(key, part):
    base = 0.02 * jax.random.normal(key, (N, N), jnp.float32)
    return (base + base.T) * 0.7071


def shard_levels(key, extent, split, low, largest):
    factor_of, own = 1.0, jax.random.fold_in(key, 6)
    for position, shards_of in split:
        heights = jnp.exp(jax.random.uniform(jax.random.fold_in(own, position), (shards_of,), jnp.float32, low / len(split), largest / len(split)))
        factor_of = factor_of * jnp.repeat(heights, extent[position] // shards_of).reshape([-1 if axis == position else 1 for axis in range(len(extent))])
    return factor_of


def scatter_about(stream_key, shape, spread, limit, cuts=(), kind=jnp.bfloat16):
    drawn = jax.random.normal(stream_key, shape, jnp.float32) * spread
    if len(cuts) > 0:
        drawn = shard_levels(stream_key, shape, cuts, -0.22, 0.18) * drawn
    return jnp.clip(drawn, min=-limit, max=limit).astype(kind)


def setup_inputs(seed: int = 0) -> dict:
    seeds = jax.random.split(jax.random.key(seed), 4)
    pair_factors = scatter_about(seeds[0], (N, AUXW), (0.5 * AUXW ** -0.5), 0.09375, ((0, 32),), jnp.float32)
    k_prev = draw_k_prev(jax.random.fold_in(seeds[3], 71), 0)
    energies = jnp.clip(jnp.exp(math.log(2.0) - 1.89712 * jax.random.uniform(seeds[2], (N,), jnp.float32) ** shard_levels(seeds[2], (N,), ((0, 8),), -0.2, 0.2)), 0.3, 2.0)
    return {"pair_factors": pair_factors, "k_prev": k_prev, "energies": energies}


def reference(pair_factors, k_prev, energies):
    coupling = k_prev + jnp.dot(pair_factors, pair_factors.T, precision=lax.Precision.HIGHEST, preferred_element_type=jnp.float32)
    casida = 4.0 * coupling + jnp.diag(energies)
    row_ids = jnp.arange(N, dtype=jnp.int32)
    col_ids = jnp.arange(PC, dtype=jnp.int32)
    upper = jnp.zeros((N, PC), jnp.float32)
    lower = jnp.zeros((N, PC), jnp.float32)
    diag_list = []
    sub_list = []
    for column_at in range(PC):
        column = casida[:, column_at] - jnp.dot(upper, lower[column_at], precision=lax.Precision.HIGHEST) - jnp.dot(lower, upper[column_at], precision=lax.Precision.HIGHEST)
        diag_list.append(column[column_at])
        below = jnp.where(row_ids > column_at, column, 0.0)
        lead = column[column_at + 1]
        sigma = jnp.sum(below * below)
        root = jnp.sqrt(sigma)
        alpha = jnp.where(lead >= 0, -root, root)
        vector = below - alpha * (row_ids == column_at + 1).astype(jnp.float32)
        length = jnp.sqrt(jnp.maximum(2.0 * (sigma + jnp.abs(lead) * root), 1.0))
        unit = vector / length
        image = jnp.dot(casida, unit, precision=lax.Precision.HIGHEST)
        image = image - jnp.dot(upper, jnp.dot(lower.T, unit, precision=lax.Precision.HIGHEST), precision=lax.Precision.HIGHEST)
        image = image - jnp.dot(lower, jnp.dot(upper.T, unit, precision=lax.Precision.HIGHEST), precision=lax.Precision.HIGHEST)
        image = 2.0 * image
        partner = image - jnp.sum(image * unit) * unit
        pick = (col_ids == column_at).astype(jnp.float32)[None, :]
        upper = upper + unit[:, None] * pick
        lower = lower + partner[:, None] * pick
        sub_list.append(alpha)
    scale = jnp.sqrt(jnp.float32(N))
    tridiagonal = jnp.stack([jnp.stack(diag_list), jnp.stack(sub_list)])
    return (casida, scale * upper, scale * lower, tridiagonal)
```

```python
import functools
import math

import jax
import jax.numpy as jnp
from jax import lax
from jax.experimental import pallas as pl
from jax.experimental.pallas import tpu as pltpu
from jax.sharding import PartitionSpec as P

PC = 8
CHUNKS = 4
LANES = 128
AXES = ("row", "col")


def walk(steps, backwards):
    order = [i ^ (i >> 1) for i in range(steps)]
    return order[:1] + order[1:][::-1] if backwards else order


def forward(moving, rows, cols, step):
    group = rows // cols
    paths = [walk(cols, member % 2 == 1) for member in range(group)]
    pairs = []
    for col in range(cols):
        for member in range(group):
            source = (col ^ paths[member][step - 1]) * group + member
            target = (col ^ paths[member][step]) * group + member
            pairs.append((source * cols + col, target * cols + col))
    return lax.ppermute(moving, AXES, pairs)


def spread_rows(mine, moved, rows, cols):
    group = rows // cols
    row_index = lax.axis_index("row")
    col_index = lax.axis_index("col")
    total = jnp.where(row_index // group == col_index, mine, jnp.zeros_like(mine))
    for part in moved:
        total = total + part
    blocks = [total]
    for shift in range(1, group):
        pairs = [
            (row, (row // group) * group + (row + shift) % group) for row in range(rows)
        ]
        blocks.append(lax.ppermute(total, "row", pairs))
    member_here = row_index % group
    ordered = []
    for member in range(group):
        block = blocks[0]
        for shift in range(1, group):
            block = jnp.where((member + shift) % group == member_here, blocks[shift], block)
        ordered.append(block)
    return jnp.concatenate(ordered, axis=0)


def total_of(value):
    return jnp.sum(value, keepdims=True).reshape(1, 1)


def householder_kernel(
    column_at, group, col_ref, panel_ref, parts_ref, upper_in, lower_in, tri_in, casida_ref,
    image_ref, upper_ref, lower_ref, tri_ref, unit_ref,
):
    rows, width = panel_ref.shape[1:]

    @pl.when(pl.program_id(0) == 0)
    def _():
        index = lax.broadcasted_iota(jnp.int32, (rows, width), 0) * width
        index = index + lax.broadcasted_iota(jnp.int32, (rows, width), 1)
        last = column_at - 1
        uppers = [upper_in[i] for i in range(column_at)]
        lowers = [lower_in[i] for i in range(max(last, 0))]
        for i in range(PC):
            upper_ref[i] = upper_in[i]
            lower_ref[i] = lower_in[i]
        if column_at > 0:
            unit = uppers[last]
            image = jnp.sum(parts_ref[...], axis=0)
            fixed = image
            for i in range(last):
                fixed = fixed - uppers[i] * total_of(lowers[i] * unit) - lowers[i] * total_of(uppers[i] * unit)
            fixed = 2.0 * fixed
            partner = fixed - total_of(fixed * unit) * unit
            lower_ref[last] = partner
            lowers.append(partner)
        if column_at < PC:
            column = panel_ref[column_at]
            here = index == column_at
            for i in range(column_at):
                at_lower = total_of(jnp.where(here, lowers[i], 0.0))
                at_upper = total_of(jnp.where(here, uppers[i], 0.0))
                column = column - uppers[i] * at_lower - lowers[i] * at_upper
            diag = total_of(jnp.where(here, column, 0.0))
            below = jnp.where(index > column_at, column, 0.0)
            head = index == column_at + 1
            lead = total_of(jnp.where(head, column, 0.0))
            sigma = total_of(below * below)
            root = jnp.sqrt(sigma)
            alpha = jnp.where(lead >= 0, -root, root)
            length = jnp.sqrt(jnp.maximum(2.0 * (sigma + jnp.abs(lead) * root), 1.0))
            unit = (below - jnp.where(head, alpha, 0.0)) / length
            upper_ref[column_at] = unit
            unit_ref[...] = unit
            lane = lax.broadcasted_iota(jnp.int32, tri_in.shape, 1)
            line = lax.broadcasted_iota(jnp.int32, tri_in.shape, 0)
            tri = tri_in[...]
            tri = jnp.where((lane == column_at) & (line == 0), diag, tri)
            tri_ref[...] = jnp.where((lane == column_at) & (line == 1), alpha, tri)
        else:
            tri_ref[...] = tri_in[...]

    if column_at < PC:
        acc = jnp.zeros((casida_ref.shape[0], LANES), jnp.float32)
        first = col_ref[0] * group
        for member in range(group):
            unit = unit_ref[pl.ds(first + member, 1), :]
            for start in range(0, width, LANES):
                at = member * width + start
                acc = acc + casida_ref[:, at : at + LANES] * unit[:, start : start + LANES]
        ones = jnp.ones((8, LANES), jnp.bfloat16)
        sums = jnp.zeros((8, casida_ref.shape[0]), jnp.float32)
        for _ in range(3):
            term = acc.astype(jnp.bfloat16)
            acc = acc - term.astype(jnp.float32)
            sums = sums + lax.dot_general(
                ones, term, (((1,), (1,)), ((), ())), preferred_element_type=jnp.float32
            )
        image_ref[...] = sums[0:1]


def householder(column_at, group, block, col, panel, parts, upper, lower, tri, casida):
    rows_here = casida.shape[0]
    last = column_at == PC
    whole = lambda x: pl.BlockSpec(x.shape, lambda i, c, n=x.ndim: (0,) * n)
    grid = (1,) if last else (rows_here // block,)
    return pl.pallas_call(
        functools.partial(householder_kernel, column_at, group),
        grid_spec=pltpu.PrefetchScalarGridSpec(
            num_scalar_prefetch=1,
            grid=grid,
            in_specs=[
                whole(panel), whole(parts), whole(upper), whole(lower), whole(tri),
                pl.BlockSpec((block, casida.shape[1]), lambda i, c: (i, 0)),
            ],
            out_specs=[
                pl.BlockSpec((1, block), lambda i, c: (0, i)),
                whole(upper), whole(lower), whole(tri),
            ],
            scratch_shapes=[pltpu.VMEM(panel.shape[1:], jnp.float32)],
        ),
        out_shape=[
            jax.ShapeDtypeStruct((1, rows_here), jnp.float32),
            jax.ShapeDtypeStruct(upper.shape, jnp.float32),
            jax.ShapeDtypeStruct(lower.shape, jnp.float32),
            jax.ShapeDtypeStruct(tri.shape, jnp.float32),
        ],
        name=f"reflect{column_at}",
    )(col, panel, parts, upper, lower, tri, casida)


def to_all(value, count):
    return lax.all_to_all(jnp.broadcast_to(value, (count,) + value.shape), AXES, 0, 0)


def shards(pair_factors, k_prev, energies):
    rows = lax.axis_size("row")
    cols = lax.axis_size("col")
    group = rows // cols
    rows_here, cols_here = k_prev.shape
    row_index = lax.axis_index("row")
    col_index = lax.axis_index("col")
    aux_here = pair_factors.shape[1]
    width = aux_here // CHUNKS
    pieces = [pair_factors[:, at : at + width] for at in range(0, aux_here, width)]
    global_rows = row_index * rows_here + jnp.arange(rows_here, dtype=jnp.int32)
    global_cols = col_index * cols_here + jnp.arange(cols_here, dtype=jnp.int32)
    on_diagonal = global_rows[:, None] == global_cols[None, :]
    casida = 4.0 * k_prev + jnp.where(on_diagonal, energies[:, None], 0.0)
    lefts = []
    moves = []
    for at, piece in enumerate(pieces):
        if at >= 2:
            first = [moves[i][at - 2 - i] for i in range(at - 1) if at - 2 - i < len(moves[i])]
            piece, first = lax.optimization_barrier((piece, first))
            for i in range(at - 1):
                if at - 2 - i < len(moves[i]):
                    moves[i][at - 2 - i] = first.pop(0)
        lefts.append(lax.all_gather(piece, "col", axis=0, tiled=True))
        moves.append([])
        for i in range(at + 1):
            if len(moves[i]) < cols - 1:
                moves[i].append(forward(moves[i][-1] if moves[i] else lefts[i], rows, cols, len(moves[i]) + 1))
    for left, moved in zip(lefts, moves):
        while len(moved) < cols - 1:
            moved.append(forward(moved[-1], rows, cols, len(moved) + 1))
        right = spread_rows(left, moved, rows, cols)
        casida = casida + lax.dot_general(
            4.0 * left, right, (((1,), (1,)), ((), ())),
            precision=lax.Precision.HIGH, preferred_element_type=jnp.float32,
        )

    lead = casida[:, :PC].T
    spread = jnp.where(col_index == 0, lead, 0.0)
    for target in range(1, cols):
        spread = spread + lax.ppermute(lead, "col", [(0, target)])
    panel = jnp.swapaxes(lax.all_gather(spread, "row", axis=0, tiled=False), 0, 1)
    upper = jnp.zeros((PC, rows, rows_here), jnp.float32)
    lower = jnp.zeros((PC, rows, rows_here), jnp.float32)
    tri = jnp.zeros((8, LANES), jnp.float32)
    parts = jnp.zeros((cols, rows, rows_here), jnp.float32)
    col = col_index.reshape(1).astype(jnp.int32)
    block = LANES * math.gcd(rows_here // LANES, 2)
    for column_at in range(PC + 1):
        image, upper, lower, tri = householder(
            column_at, group, block, col, panel, parts, upper, lower, tri, casida
        )
        if column_at < PC:
            parts = to_all(image.reshape(rows_here), rows * cols)
            parts = jnp.swapaxes(parts.reshape(rows, cols, rows_here), 0, 1)
    scale = jnp.sqrt(jnp.float32(rows * rows_here))
    pick = lambda x: scale * lax.dynamic_index_in_dim(x, row_index, 1, keepdims=False).T
    return (casida, pick(upper), pick(lower), tri[:2, :PC])


def solution(mesh):
    in_specs = (P(("row", "col"), None), P("row", "col"), P("row"))
    out_specs = (P("row", "col"), P("row", None), P("row", None), P())
    return jax.shard_map(shards, mesh=mesh, in_specs=in_specs, out_specs=out_specs, check_vma=False)
```
